256 devices in a mesh: row: 128 (over z, y, x), width: 2 (over core).
Axes of the slice: x: 4, y: 4, z: 8, core: 2. Of those that a mesh axis runs over, the one named last changes fastest.
Arguments:
- row_numbers: int32 [4096, 2], P('row'), may hold values from 0 to 131071
- item_table: bfloat16 [131072, 64], P('row', 'width'), may hold values from -6 to 6
- dense_part: float32 [4096, 64], P('row', 'width'), may hold values from -6 to 6
- small_ids: int32 [4096], P('row'), may hold values from 0 to 255
- small_table: bfloat16 [256, 64], P('row', 'width'), may hold values from -6 to 6
Outputs:
- features: bfloat16 [4096, 3, 64], P('row', None, 'width')
The draws below stay inside these ranges and needn't reach their ends.
All inputs are finite; a program needn't handle non-finite values.
Results may differ from the reference program's by a relative error of at most 0.0004.
Values may be sent and summed in bfloat16 or wider, within the bound.
A program may use at most 64 MiB of HBM per device.

```python
import math
import jax
import jax.numpy as jnp
import numpy as np

EXAMPLES = 4096
FEATURES = 64
PICKS = 2
BIG_ROWS = 131072
SMALL_ROWS = 256


def place_ends(entries, stream_key, least, largest):
    spot = [jax.random.randint(jax.random.fold_in(stream_key, axis), (), 0, length) for axis, length in enumerate(entries.shape)]
    widest = entries.shape.index(max(entries.shape))
    neighbour = spot[:widest] + [(spot[widest] + 1) % entries.shape[widest]] + spot[widest + 1:]
    return entries.at[tuple(spot)].set(least).at[tuple(neighbour)].set(largest)


def block_levels(rng, dims, split, low, top_value):
    loudness, own = 1.0, jax.random.fold_in(rng, 6)
    for dim, blocks in split:
        heights = jnp.exp(jax.random.uniform(jax.random.fold_in(own, dim), (blocks,), jnp.float32, low / len(split), top_value / len(split)))
        loudness = loudness * jnp.repeat(heights, dims[dim] // blocks).reshape([-1 if axis == dim else 1 for axis in range(len(dims))])
    return loudness


def wide_ids(key, shape, amount, skew):
    portions = [min(1 << octave, amount + 1 - (1 << octave)) * (1 << 20) // math.isqrt((1 << octave) ** skew) + 1 for octave in range((amount + 1).bit_length()) if 1 << octave <= amount]
    spread = 1 + sum(portions) // (1 << 30)
    table = np.cumsum(np.array([max(1, weight // spread) for weight in portions]))
    lot = jax.random.randint(jax.random.fold_in(key, 1), shape, 0, int(table[len(portions) - 1]))
    start = jnp.left_shift(1, jnp.searchsorted(jnp.asarray(table, jnp.int32), lot, side="right").astype(jnp.int32))
    standing = start - 1 + jax.random.randint(jax.random.fold_in(key, 4), shape, 0, 1 << 30) % jnp.minimum(start, amount + 1 - start)
    return jax.random.permutation(jax.random.fold_in(key, 2), amount)[standing].astype(jnp.int32)


def noise(stream_key, extent, deviation, most, shards=(), kind=jnp.bfloat16):
    values = deviation * jax.random.normal(stream_key, extent, jnp.float32)
    if shards:
        values = values * block_levels(stream_key, extent, shards, -0.22, 0.18)
    return jnp.clip(values, -most, most).astype(kind)


def setup_inputs(seed: int = 0) -> dict:
    splits = jax.random.split(jax.random.key(seed), 6)
    row_numbers = place_ends(wide_ids(splits[0], (EXAMPLES, PICKS), BIG_ROWS, 2), jax.random.fold_in(splits[0], 3), 0, BIG_ROWS - 1).astype(jnp.int32)
    item_table = noise(splits[1], (BIG_ROWS, FEATURES), 1.0, 6.0, ((0, 128), (1, 2)))
    dense_part = noise(splits[2], (EXAMPLES, FEATURES), 1.0, 6.0, ((0, 128), (1, 2)), jnp.float32)
    small_ids = place_ends(jax.random.randint(splits[3], (EXAMPLES,), 0, SMALL_ROWS), jax.random.fold_in(splits[3], 1), 0, SMALL_ROWS - 1).astype(jnp.int32)
    small_table = noise(splits[4], (SMALL_ROWS, FEATURES), 1.0, 6.0, ((0, 128), (1, 2)))
    return {"row_numbers": row_numbers, "item_table": item_table, "dense_part": dense_part, "small_ids": small_ids, "small_table": small_table}


def reference(row_numbers, item_table, dense_part, small_ids, small_table):
    pooled = jnp.sum(item_table[row_numbers].astype(jnp.float32), axis=1) * PICKS ** -0.5
    small_rows = small_table[small_ids].astype(jnp.float32)
    features = jnp.stack([dense_part, pooled, small_rows], axis=1).astype(jnp.bfloat16)
    return features
```

```python
import functools

import jax
import jax.numpy as jnp
from jax import lax
from jax.experimental import pallas as pl
from jax.experimental.pallas import tpu as pltpu
from jax.sharding import PartitionSpec as P

MESH = pl.DeviceIdType.MESH
LANES = 128
GROUP = 256


def masks(bits):
    out = [0]
    for bit in bits:
        out = out + [m | 1 << bit for m in out]
    return out


def drain(view, sem):
    pltpu.make_async_copy(view, view, sem).wait()


def kernel(
    near_masks, far_masks, scale,
    ids_hbm, table_hbm, dense_hbm, small_ids_hbm, small_hbm, out_ref,
    ids, tables, dense, small_ids, smalls, packed, arrived,
    local_sem, send_sem, ids_sem, table_sem, small_sem, far_sem, value_sem,
):
    me = lax.axis_index("row")
    near, far = len(near_masks), len(far_masks)
    picks, examples = ids.shape[1:]
    features, rows = tables.shape[1:]
    span = smalls.shape[2]
    per_tile = LANES // examples
    tiles = far // per_tile
    chunks = rows // GROUP

    def peer(mask):
        return {"row": me ^ mask}

    barrier = pltpu.get_barrier_semaphore()
    for mask in [*reversed(far_masks[1:]), *reversed(near_masks[1:])]:
        pl.semaphore_signal(barrier, inc=1, device_id=peer(mask), device_id_type=MESH)

    own = [
        pltpu.make_async_copy(src, dst, local_sem.at[i])
        for i, (src, dst) in enumerate(
            [
                (ids_hbm, ids.at[0]),
                (small_hbm, smalls.at[0, 0]),
                (table_hbm, tables.at[0]),
                (dense_hbm, dense),
                (small_ids_hbm, small_ids),
            ]
        )
    ]
    for copy in own:
        copy.start()

    def remote(src, dst, kind, arrival, mask):
        return pltpu.make_async_remote_copy(
            src_ref=src, dst_ref=dst, send_sem=send_sem.at[kind], recv_sem=arrival,
            device_id=peer(mask), device_id_type=MESH,
        )

    with jax.named_scope("barrier"):
        own[0].wait()
        pl.semaphore_wait(barrier, far - 1 + near - 1)
    for s in reversed(range(1, far)):
        remote(ids.at[0], ids.at[s], 0, ids_sem.at[s // per_tile], far_masks[s]).start()
    own[1].wait()
    for s in range(1, near):
        remote(smalls.at[0, 0], smalls.at[0, s], 1, small_sem, near_masks[s]).start()
    own[2].wait()
    for s in reversed(range(1, near)):
        remote(tables.at[0], tables.at[s], 2, table_sem.at[s], near_masks[s]).start()

    own[3].wait()
    own[4].wait()
    out_ref[0] = dense[...].astype(out_ref.dtype)

    with jax.named_scope("smallnear"):
        drain(smalls.at[0, pl.ds(1, near - 1)], small_sem)
    for s in reversed(range(1, far)):
        remote(smalls.at[0], smalls.at[s], 3, far_sem, far_masks[s]).start()

    with jax.named_scope("idswait"):
        drain(ids.at[pl.ds(1, per_tile - 1)], ids_sem.at[0])
        for k in range(1, tiles):
            drain(ids.at[pl.ds(k * per_tile, per_tile)], ids_sem.at[k])
    with jax.named_scope("tabwait"):
        for s in range(1, near):
            drain(tables.at[s], table_sem.at[s])

    near_bits = near_masks[-1]
    spot = lax.broadcasted_iota(jnp.int32, (GROUP, LANES), 0)
    stack = jnp.concatenate(
        [tables[t, :, c * GROUP : (c + 1) * GROUP] for t in range(near) for c in range(chunks)], axis=0
    )
    with jax.named_scope("compute"):
        for k in reversed(range(tiles)):
            wanted = jnp.concatenate(
                [ids[k * per_tile + i] for i in range(per_tile)], axis=1
            )
            low = wanted % GROUP
            chunk = wanted // GROUP % chunks
            owner = (wanted // rows) ^ me
            hits = jnp.concatenate(
                [
                    jnp.where(spot == low[p : p + 1], 1.0, 0.0).astype(tables.dtype)
                    for p in range(picks)
                ],
                axis=1,
            )
            found = jnp.dot(stack, hits, preferred_element_type=jnp.float32)
            total = jnp.zeros((features, LANES), jnp.float32)
            for p in range(picks):
                chosen = jnp.zeros((features, LANES), jnp.float32)
                for t in range(near):
                    for c in range(chunks):
                        j = t * chunks + c
                        want = owner[p : p + 1] * chunks + chunk[p : p + 1]
                        chosen = jnp.where(
                            want == near_masks[t] * chunks + c,
                            found[j * features : (j + 1) * features, p * LANES : (p + 1) * LANES],
                            chosen,
                        )
                total = total + chosen
            for i in reversed(range(per_tile)):
                s = k * per_tile + i
                packed[s] = jnp.concatenate(
                    [
                        total[8 * b : 8 * b + 8, i * examples : (i + 1) * examples]
                        for b in range(features // 8)
                    ],
                    axis=1,
                )
                if s:
                    remote(packed.at[s], arrived.at[s], 4, value_sem, far_masks[s]).start()

    with jax.named_scope("smallwait"):
        drain(smalls.at[pl.ds(1, far - 1)], far_sem)
    with jax.named_scope("rows"):
        column = jnp.broadcast_to(small_ids[...], (8, examples)).T[:, 0:1]
        place = jnp.broadcast_to(column ^ (me * span), (examples, features))
        rows_out = jnp.zeros((examples, features), jnp.float32)
        for f in range(far):
            for n in range(near):
                part = smalls[f, n].astype(jnp.float32)
                for r in range(span):
                    rows_out = jnp.where(
                        place == (far_masks[f] | near_masks[n]) * span + r, part[r : r + 1], rows_out
                    )
        out_ref[2] = rows_out.astype(out_ref.dtype)

    with jax.named_scope("valwait"):
        drain(arrived.at[pl.ds(1, far - 1)], value_sem)
    total = packed[0]
    for s in range(1, far):
        total = total + arrived[s]
    total = total * scale
    pooled = jnp.concatenate(
        [total[:, b * examples : (b + 1) * examples] for b in range(features // 8)], axis=0
    ).T
    out_ref[1] = pooled.astype(out_ref.dtype)

    with jax.named_scope("sendwait"):
        drain(ids.at[pl.ds(1, far - 1)], send_sem.at[0])
        drain(smalls.at[0, pl.ds(1, near - 1)], send_sem.at[1])
        drain(tables.at[pl.ds(1, near - 1)], send_sem.at[2])
        drain(smalls.at[pl.ds(1, far - 1)], send_sem.at[3])
        drain(packed.at[pl.ds(1, far - 1)], send_sem.at[4])


def per_device(near_bits, far_bits, row_numbers, item_table, dense_part, small_ids, small_table):
    near_masks, far_masks = masks(near_bits), masks(far_bits)
    near, far = len(near_masks), len(far_masks)
    examples, picks = row_numbers.shape
    rows, features = item_table.shape
    tiles = far * examples // LANES
    dma = pltpu.SemaphoreType.DMA
    out = pl.pallas_call(
        functools.partial(kernel, near_masks, far_masks, picks ** (-0.5)),
        out_shape=pltpu.VMEM((3, examples, features), jnp.bfloat16),
        in_specs=[pl.BlockSpec(memory_space=pl.ANY)] * 5,
        out_specs=pl.BlockSpec(memory_space=pltpu.VMEM),
        scratch_shapes=[
            pltpu.VMEM((far, picks, examples), jnp.int32),
            pltpu.VMEM((near, features, rows), item_table.dtype),
            pltpu.VMEM(dense_part.shape, dense_part.dtype),
            pltpu.VMEM((1, examples), jnp.int32),
            pltpu.VMEM((far, near) + small_table.shape, small_table.dtype),
            pltpu.VMEM((far, 8, features // 8 * examples), jnp.float32),
            pltpu.VMEM((far, 8, features // 8 * examples), jnp.float32),
            dma((5,)), dma((5,)), dma((tiles,)), dma((near,)), dma, dma, dma,
        ],
        compiler_params=pltpu.CompilerParams(collective_id=0, has_side_effects=True),
    )(row_numbers.T, item_table.T, dense_part, small_ids[None, :], small_table)
    return jnp.transpose(out, (1, 0, 2))


NEAR = (2, 3)
FAR = (0, 1, 4, 5, 6)


def solution(mesh):
    placed = (P("row", None), P("row", "width"), P("row", "width"), P("row"), P("row", "width"))
    return jax.shard_map(
        functools.partial(per_device, NEAR, FAR),
        mesh=mesh, in_specs=placed, out_specs=P("row", None, "width"), check_vma=False,
    )
```
